512 devices in a mesh: seq: 64 (over z, y), head: 8 (over x, core).
Axes of the slice: x: 4, y: 8, z: 8, core: 2. Of those that a mesh axis runs over, the one named last changes fastest.
Arguments:
- queries: bfloat16 [16384, 32, 128], P('seq', 'head'), may hold values from -8 to 8
- keys: bfloat16 [16384, 8, 128], P('seq', 'head'), may hold values from -8 to 8
- values: bfloat16 [16384, 8, 128], P('seq', 'head'), may hold values from -6 to 6
- out_weight: bfloat16 [4096, 4096], P('head', 'seq'), may hold values from -0.25 to 0.25
- doc_lengths: int32 [64], replicated, may hold values from 1 to 8448, 16384 in all
Outputs:
- projected: bfloat16 [16384, 4096], P('seq', 'head')
The draws below stay inside these ranges and needn't reach their ends.
Inputs may be any that keep to these rules, and one draw needn't show every extreme that they name: `doc_lengths`: every document is at most 8448 tokens long and the longest is exactly that; the lengths sum to 16384.
All inputs are finite; a program needn't handle non-finite values.
Results may differ from the reference program's by a relative error of at most 0.014.
Values may be sent and summed in bfloat16 or wider, within the bound.
No kernel may reach another device: no remote copies, remote signals or barrier semaphores. Data moves between devices by JAX's collectives and lax.ppermute only.
A program may use at most 64 MiB of HBM per device.

```python
import math
import jax
import jax.numpy as jnp
import numpy as np
from jax import lax

D = 4096
H = 32
KVH = 8
HD = 128
TOK_DEV = 256
REACH = 33
TOKENS = 16384
NDOCS = 64
N_HEAD = 8


def drawn_draws(base_key):
    first_key, second_key = jax.random.split(base_key, 2)
    queries = jnp.clip(jax.random.normal(first_key, (TOKENS, H, HD)), -8.0, 8.0)
    keys = jnp.clip(jax.random.normal(second_key, (TOKENS, KVH, HD)), -8.0, 8.0)
    return (queries, keys)


def draw_queries(key, part):
    queries, keys = drawn_draws(jax.random.fold_in(key, 7))
    return queries.astype(jnp.bfloat16)


def draw_keys(key, part):
    queries, keys = drawn_draws(jax.random.fold_in(key, 7))
    return keys.astype(jnp.bfloat16)


def with_spikes(result, own_key, source, target, blocks, factor):
    owner, partner = [(jnp.arange(result.shape[dim]) // (result.shape[dim] // blocks)).reshape([-1 if axis == dim else 1 for axis in range(result.ndim)]) for dim in (source, target)]
    chosen = jax.random.permutation(own_key, blocks)[partner]
    strong = (owner == chosen) | (owner == (partner + blocks // 2) % blocks)
    return jnp.where(strong, factor * result, result)


def shard_levels(own_key, dims, pieces, smallest, largest):
    gain = 1.0
    for dim, parts in pieces:
        draws = jax.random.uniform(jax.random.fold_in(jax.random.fold_in(own_key, 6), dim), (parts,), jnp.float32, smallest / len(pieces), largest / len(pieces))
        gain = gain * jnp.repeat(jnp.exp(draws), dims[dim] // parts).reshape((-1,) + (1,) * (len(dims) - 1 - dim))
    return gain


def length_profile(count, total, bound, lean):
    portions = [(1 << 20) // math.isqrt(standing ** lean) + 1 for standing in range(2, count + 1)]
    spare, given = total - bound - (count - 1), [1] * (count - 1)
    while spare > 0:
        candidates = [i for i in range(count - 1) if given[i] < bound]
        mass, remaining = sum([portions[i] for i in candidates]), spare
        for i in candidates:
            extra = min(bound - given[i], max(1, remaining * portions[i] // mass), spare)
            given[i] = given[i] + extra
            spare = spare - extra
    return np.array([bound] + given)


def uneven_parts(key, count, total, most, lean):
    if count == 2:
        one = jax.random.randint(key, (), max(1, total - most), min(most, total - 1) + 1)
        return jnp.stack([one, total - one])
    sizes = jnp.asarray(length_profile(count, total, most, lean), jnp.int32)
    twos = (count - 1) // 2
    donor, taker = sizes[1:1 + 2 * twos:2], sizes[2:2 + 2 * twos:2]
    room = jnp.minimum(donor - 1, most - taker)
    passed = jax.random.randint(jax.random.fold_in(key, 1), (twos,), 0, 1 << 20) % (room + 1)
    sizes = sizes.at[1:1 + 2 * twos:2].set(donor - passed).at[2:2 + 2 * twos:2].set(taker + passed)
    return sizes[jax.random.permutation(jax.random.fold_in(key, 2), count)]


def centred(stream_key, extent, width, limit, shards=(), held_as=jnp.bfloat16):
    loudness = shard_levels(stream_key, extent, shards, -0.22, 0.18) if shards else 1.0
    values = jax.random.normal(stream_key, extent, jnp.float32) * width * loudness
    return jnp.minimum(jnp.maximum(values, -limit), limit).astype(held_as)


def heavy_noise(own_key, dims, deviation, most, cuts, heavy, kind=jnp.bfloat16):
    array = deviation * jax.random.normal(own_key, dims, jnp.float32)
    if cuts:
        array = array * shard_levels(own_key, dims, cuts, -0.22, 0.18)
    return jnp.clip(with_spikes(array, jax.random.fold_in(own_key, 3), *heavy), -most, most).astype(kind)


def setup_inputs(seed: int = 0) -> dict:
    seeds = jax.random.split(jax.random.key(seed), 6)
    return {
        "queries": draw_queries(jax.random.fold_in(seeds[5], 71), 0),
        "keys": draw_keys(jax.random.fold_in(seeds[5], 71), 0),
        "values": centred(seeds[2], (TOKENS, KVH, HD), 1.0, 6.0, ((0, 64), (1, 8))),
        "out_weight": heavy_noise(seeds[3], (H * HD, D), (H * HD) ** -0.5, 0.25, ((0, 8), (1, 64)), (0, 1, 64, 4.0)),
        "doc_lengths": uneven_parts(seeds[4], NDOCS, TOKENS, REACH * TOK_DEV, 2).astype(jnp.int32),
    }


def doc_index(positions, doc_lengths):
    doc_ends = jnp.cumsum(doc_lengths)
    return jnp.sum((doc_ends[None, :] <= positions[:, None]).astype(jnp.int32), axis=1)


def reference(queries, keys, values, out_weight, doc_lengths):
    block_rows = TOK_DEV
    window = REACH * TOK_DEV
    group_size = H // KVH
    score_scale = 1.0 / (HD ** 0.5)
    positions = jnp.arange(TOKENS, dtype=jnp.int32)
    docs = doc_index(positions, doc_lengths)
    key_padded = jnp.concatenate([jnp.zeros((window, KVH, HD), jnp.bfloat16), keys], axis=0)
    value_padded = jnp.concatenate([jnp.zeros((window, KVH, HD), jnp.bfloat16), values], axis=0)
    doc_padded = jnp.concatenate([jnp.full((window,), -1, jnp.int32), docs], axis=0)

    def one_block(block_index):
        first_row = (block_index * block_rows).astype(jnp.int32)
        query_rows = lax.dynamic_slice_in_dim(queries, first_row, block_rows, 0)
        query_rows = query_rows.reshape(block_rows, KVH, group_size, HD).astype(jnp.float32)
        key_rows = lax.dynamic_slice_in_dim(key_padded, first_row, window + block_rows, 0).astype(jnp.float32)
        value_rows = lax.dynamic_slice_in_dim(value_padded, first_row, window + block_rows, 0).astype(jnp.float32)
        key_doc = lax.dynamic_slice_in_dim(doc_padded, first_row, window + block_rows, 0)
        query_doc = lax.dynamic_slice_in_dim(docs, first_row, block_rows, 0)
        key_pos = first_row - window + jnp.arange(window + block_rows, dtype=jnp.int32)
        query_pos = first_row + jnp.arange(block_rows, dtype=jnp.int32)
        allowed = (key_pos[None, :] >= 0) & (key_pos[None, :] <= query_pos[:, None]) & (key_doc[None, :] == query_doc[:, None])
        scores = jnp.einsum("qgrd,kgd->grqk", query_rows, key_rows) * score_scale
        scores = jnp.where(allowed, scores, -1e30)
        row_max = jnp.max(scores, axis=3)
        expo = jnp.where(allowed, jnp.exp(scores - row_max[..., None]), 0.0)
        row_total = jnp.sum(expo, axis=3)
        rounded = lax.optimization_barrier(expo.astype(jnp.bfloat16))
        output = jnp.einsum("grqk,kgd->grqd", rounded.astype(jnp.float32), value_rows) / row_total[..., None]
        return jnp.transpose(output, (2, 0, 1, 3)).reshape(block_rows, H * HD).astype(jnp.bfloat16)

    attended = lax.map(one_block, jnp.arange(TOKENS // TOK_DEV, dtype=jnp.int32)).reshape(TOKENS, H * HD)
    group_rows = H * HD // N_HEAD
    summed = jnp.zeros((TOKENS, D), jnp.float32)
    for group_index in range(N_HEAD):
        partial_value = jnp.dot(attended[:, group_index * group_rows:(group_index + 1) * group_rows],
                          out_weight[group_index * group_rows:(group_index + 1) * group_rows],
                          preferred_element_type=jnp.float32).astype(jnp.bfloat16)
        partial_value = lax.optimization_barrier(partial_value)
        summed = summed + partial_value.astype(jnp.float32)
    return summed.astype(jnp.bfloat16)
```

```python
import math

import jax
import jax.numpy as jnp
from jax import lax
from jax.experimental import pallas as pl
from jax.experimental.pallas import tpu as pltpu
from jax.sharding import PartitionSpec as P

NEG = -1e30
CHUNK = 4


def attend_and_project(where, queries, starts, packed, blocks, tok, heads, width):
    factor = math.log2(math.e) / math.sqrt(width)
    span = CHUNK * tok
    pieces = blocks // 8
    wrows = packed.shape[1] - 2 * tok
    wcols = wrows // heads

    def kernel(where_ref, q_ref, starts_ref, packed_ref, out_ref, kv, wbuf, accum, top, sems, wsem):
        me, first, last_start, core = where_ref[0], where_ref[1], where_ref[2], where_ref[3]
        count = (me - first) // CHUNK + 1

        def fetch(step):
            block = jnp.minimum(first + CHUNK * step, blocks - CHUNK)
            slot = lax.rem(step, 2)
            return pltpu.make_async_copy(
                packed_ref.at[pl.ds(block, CHUNK), pl.ds(0, 2 * tok), :], kv.at[slot], sems.at[slot]
            )

        fetch(0).start()
        weights_copy = pltpu.make_async_copy(packed_ref.at[:, pl.ds(2 * tok, wrows), :], wbuf, wsem)
        weights_copy.start()
        accum[...] = jnp.zeros_like(accum)
        top[...] = jnp.full_like(top, NEG)
        ones = jnp.ones((span, width), jnp.bfloat16)

        def turn(step, nothing):
            slot = lax.rem(step, 2)
            fetch(step).wait()

            @pl.when(step + 1 < count)
            def _():
                fetch(step + 1).start()

            wanted = first + CHUNK * step
            base = jnp.minimum(wanted, blocks - CHUNK) * tok

            def process(masked):
                keys = kv[slot, :, :tok, :].reshape(span, width)
                vals = kv[slot, :, tok:, :].reshape(span, width)
                vals = jnp.concatenate([vals, ones], axis=1)
                if masked:
                    key_pos = base + lax.broadcasted_iota(jnp.int32, (tok, span), 1)
                    query_pos = me * tok + lax.broadcasted_iota(jnp.int32, (tok, span), 0)
                    lowest = jnp.maximum(starts_ref[:, :1], wanted * tok)
                    allowed = (key_pos >= lowest) & (key_pos <= query_pos)
                for h in range(heads):
                    scores = lax.dot_general(
                        q_ref[h], keys, (((1,), (1,)), ((), ())), preferred_element_type=jnp.float32
                    )
                    if masked:
                        scores = jnp.where(allowed, scores, NEG)
                    old = top[h][:, :1]
                    new = jnp.maximum(old, jnp.max(scores, axis=1, keepdims=True))
                    weights = jnp.exp2((scores - new) * factor).astype(jnp.bfloat16)
                    rescale = jnp.exp2((old - new) * factor)
                    accum[h] = accum[h] * rescale + jnp.dot(
                        weights, vals, preferred_element_type=jnp.float32
                    )
                    top[h] = jnp.broadcast_to(new, (tok, width))

            full = (base + span - 1 <= me * tok) & (base >= last_start)
            pl.when(full)(lambda: process(False))
            pl.when(jnp.logical_not(full))(lambda: process(True))
            return nothing

        lax.fori_loop(0, count, turn, 0)
        attended = jnp.concatenate(
            [(accum[h][:, :width] / accum[h][:, width:]).astype(jnp.bfloat16) for h in range(heads)], axis=1
        )
        weights_copy.wait()
        for kept in range(2):
            for x in range(4):
                owner = 2 * x + jnp.where(kept == 0, core, 1 - core)
                part = wbuf[pl.ds(owner * pieces, pieces)]
                part = jnp.concatenate(
                    [
                        part[:, h * wcols : (h + 1) * wcols, :].reshape(pieces * wcols, width)
                        for h in range(heads)
                    ],
                    axis=1,
                )
                out_ref[kept, x] = lax.dot_general(
                    attended, part, (((1,), (1,)), ((), ())), preferred_element_type=jnp.float32
                ).astype(jnp.bfloat16)

    return pl.pallas_call(
        kernel,
        out_shape=jax.ShapeDtypeStruct((2, 4, tok, pieces * wcols), jnp.bfloat16),
        in_specs=[
            pl.BlockSpec(memory_space=pltpu.SMEM),
            pl.BlockSpec(memory_space=pltpu.VMEM),
            pl.BlockSpec(memory_space=pltpu.VMEM),
            pl.BlockSpec(memory_space=pl.ANY),
        ],
        out_specs=pl.BlockSpec(memory_space=pltpu.VMEM),
        scratch_shapes=[
            pltpu.VMEM((2, CHUNK, 2 * tok, width), jnp.bfloat16),
            pltpu.VMEM((blocks, wrows, width), jnp.bfloat16),
            pltpu.VMEM((heads, tok, 2 * width), jnp.float32),
            pltpu.VMEM((heads, tok, width), jnp.float32),
            pltpu.SemaphoreType.DMA((2,)),
            pltpu.SemaphoreType.DMA,
        ],
        compiler_params=pltpu.CompilerParams(vmem_limit_bytes=40 * 1024 * 1024),
        name="attend",
    )(where, queries, starts, packed)


def body(queries, keys, values, out_weight, doc_lengths):
    tok, heads, width = queries.shape
    blocks = lax.axis_size("seq")
    me = lax.axis_index("seq")
    core = lax.axis_index("head") % 2
    turned = out_weight.T
    packed = jnp.concatenate(
        [keys.reshape(tok, width), values.reshape(tok, width)]
        + [turned[:, h * width : (h + 1) * width] for h in range(heads)],
        axis=0,
    )
    packed = lax.all_gather(packed, "seq", axis=0)

    ends = jnp.cumsum(doc_lengths)
    position = me * tok + jnp.arange(tok, dtype=jnp.int32)
    starts = jnp.max(jnp.where(ends[None, :] <= position[:, None], ends[None, :], 0), axis=1)
    where = jnp.stack([me, starts[0] // tok, starts[-1], core]).astype(jnp.int32)
    starts = jnp.broadcast_to(starts[:, None], (tok, 128))
    partial = attend_and_project(
        where, jnp.transpose(queries, (1, 0, 2)), starts, packed, blocks, tok, heads, width
    )
    pairs = [(h, h ^ 1) for h in range(8)]
    other = lax.ppermute(partial[1], "head", pairs)
    both = (partial[0].astype(jnp.float32) + other.astype(jnp.float32)).astype(jnp.bfloat16)
    parts = lax.all_to_all(
        both, "head", 0, 0, axis_index_groups=[[0, 2, 4, 6], [1, 3, 5, 7]], tiled=True
    )
    return jnp.sum(parts.astype(jnp.float32), axis=0).astype(jnp.bfloat16)


def solution(mesh):
    placed = (
        P("seq", "head", None),
        P("seq", "head", None),
        P("seq", "head", None),
        P("head", "seq"),
        P(),
    )
    return jax.shard_map(
        body, mesh=mesh, in_specs=placed, out_specs=P("seq", "head"), check_vma=False
    )
```

```python
import math

import jax
import jax.numpy as jnp
from jax import lax
from jax.experimental import pallas as pl
from jax.experimental.pallas import tpu as pltpu
from jax.sharding import PartitionSpec as P


NEG = -1e30


def visit(where_ref, q_ref, starts_ref, block_ref, offsets, accum, top):
    heads, tok, width = q_ref.shape
    factor = math.log2(math.e) / math.sqrt(width)
    span = len(offsets) * tok
    me, first, last_start = where_ref[0], where_ref[1], where_ref[2]

    def process(masked):
        keys = block_ref[:, :tok, :].reshape(span, width)
        vals = block_ref[:, tok:, :].reshape(span, width)
        vals = jnp.concatenate([vals, jnp.ones((span, width), jnp.bfloat16)], axis=1)
        if masked:
            lane = lax.broadcasted_iota(jnp.int32, (1, tok), 1)
            key_pos = jnp.concatenate([lane + (me + offset) * tok for offset in offsets], axis=1)
            query_pos = me * tok + lax.broadcasted_iota(jnp.int32, (tok, 1), 0)
            allowed = (key_pos >= starts_ref[:, :1]) & (key_pos <= query_pos)

        def one_head(h):
            scores = lax.dot_general(
                q_ref[h], keys, (((1,), (1,)), ((), ())), preferred_element_type=jnp.float32
            )
            if masked:
                scores = jnp.where(allowed, scores, NEG)
            old = top[h][:, :1]
            new = jnp.maximum(old, jnp.max(scores, axis=1, keepdims=True))
            weights = jnp.exp2((scores - new) * factor).astype(jnp.bfloat16)
            rescale = jnp.exp2((old - new) * factor)
            accum[h] = accum[h] * rescale + jnp.dot(weights, vals, preferred_element_type=jnp.float32)
            top[h] = jnp.broadcast_to(new, (tok, width))

        if masked:
            pl.loop(0, heads)(one_head)
        else:
            for h in range(heads):
                one_head(h)

    needed = me + max(offsets) >= first
    full = ((me + min(offsets)) * tok >= last_start) & (max(offsets) < 0)
    pl.when(needed & full)(lambda: process(False))
    pl.when(needed & jnp.logical_not(full))(lambda: process(True))


def attend(where, queries, starts, sets, state, weight=None):
    heads, tok, width = queries.shape
    arrays = [array for array, _ in sets]
    offsets = [offset for _, offset in sets]
    count = len(sets)
    state_shapes = [
        jax.ShapeDtypeStruct((heads, tok, 2 * width), jnp.float32),
        jax.ShapeDtypeStruct((heads, tok, width), jnp.float32),
    ]
    vmem = pl.BlockSpec(memory_space=pltpu.VMEM)
    specs = [pl.BlockSpec(memory_space=pltpu.SMEM)] + [vmem] * (2 + count)
    keys_seen = sum(map(len, offsets)) * tok
    cost = pl.CostEstimate(
        flops=4 * heads * tok * keys_seen * width,
        bytes_accessed=4 * keys_seen * width,
        transcendentals=heads * tok * keys_seen,
    )
    limit = pltpu.CompilerParams(vmem_limit_bytes=32 * 1024 * 1024)

    if weight is None:

        def kernel(where_ref, q_ref, starts_ref, *refs):
            blocks = refs[:count]
            accum, top = refs[-2:]
            if state is None:
                accum[...] = jnp.zeros_like(accum)
                top[...] = jnp.full_like(top, NEG)
            for block, offset in zip(blocks, offsets):
                visit(where_ref, q_ref, starts_ref, block, offset, accum, top)

        given = [] if state is None else list(state)
        return pl.pallas_call(
            kernel,
            out_shape=state_shapes,
            in_specs=specs + [vmem] * len(given),
            out_specs=[vmem, vmem],
            input_output_aliases={} if state is None else {3 + count: 0, 4 + count: 1},
            compiler_params=limit,
            cost_estimate=cost,
            name="attend",
        )(where, queries, starts, *arrays, *given)

    cols = weight.shape[0] // 8

    def last(where_ref, q_ref, starts_ref, *refs):
        blocks = refs[:count]
        accum_in, top_in, weight_ref, out_ref, accum, top, wbuf, sem = refs[count:]
        copy = pltpu.make_async_copy(weight_ref, wbuf, sem)
        copy.start()
        accum[...] = accum_in[...]
        top[...] = top_in[...]
        for block, offset in zip(blocks, offsets):
            visit(where_ref, q_ref, starts_ref, block, offset, accum, top)
        attended = jnp.concatenate(
            [(accum[h][:, :width] / accum[h][:, width:]).astype(jnp.bfloat16) for h in range(heads)], axis=1
        )
        copy.wait()
        core = where_ref[3]
        for kept in range(2):
            for x in range(4):
                owner = 2 * x + (core if kept == 0 else 1 - core)
                part = wbuf[pl.ds(pl.multiple_of(owner * cols, cols), cols), :]
                out_ref[kept, x] = lax.dot_general(
                    attended, part, (((1,), (1,)), ((), ())), preferred_element_type=jnp.float32
                ).astype(jnp.bfloat16)

    return pl.pallas_call(
        last,
        out_shape=jax.ShapeDtypeStruct((2, 4, tok, cols), jnp.bfloat16),
        in_specs=specs + [vmem, vmem, pl.BlockSpec(memory_space=pltpu.HBM)],
        out_specs=vmem,
        scratch_shapes=[
            pltpu.VMEM((heads, tok, 2 * width), jnp.float32),
            pltpu.VMEM((heads, tok, width), jnp.float32),
            pltpu.VMEM(weight.shape, jnp.bfloat16),
            pltpu.SemaphoreType.DMA,
        ],
        compiler_params=limit,
        cost_estimate=cost,
        name="finish",
    )(where, queries, starts, *arrays, *state, weight)


def moved(array, steps):
    count = lax.axis_size("seq")
    return lax.ppermute(array, "seq", [(i, (i + steps) % count) for i in range(count)])


def layer(queries, keys, values, out_weight, doc_lengths):
    tok, _, width = queries.shape
    me = lax.axis_index("seq")
    core = lax.axis_index("head") % 2
    weight = lax.all_gather(out_weight.T, "seq", axis=0, tiled=True)

    own = jnp.concatenate([keys.reshape(1, tok, width), values.reshape(1, tok, width)], axis=1)
    column = jnp.concatenate([own] + [moved(own, 8 * a) for a in (1, 2, 3, 4)], axis=0)

    ends = jnp.cumsum(doc_lengths)
    position = me * tok + jnp.arange(tok, dtype=jnp.int32)
    starts = jnp.max(jnp.where(ends[None, :] <= position[:, None], ends[None, :], 0), axis=1)
    where = jnp.stack([me, starts[0] // tok, starts[-1], core]).astype(jnp.int32)
    starts = jnp.broadcast_to(starts[:, None], (tok, 128))
    turned = jnp.transpose(queries, (1, 0, 2))

    sets, state = [(column, [-8 * a for a in range(5)])], None
    up, down = column, column[1:]
    for turn in range(1, 5):
        up = moved(up if turn == 1 else up[:4] if turn < 4 else up[:2], 1)
        down = moved(down if turn < 4 else down[2:], -1)
        state = attend(where, turned, starts, sets, state)
        below = [-turn - 8 * a for a in range(up.shape[0])]
        above = [turn - 8 * a for a in range(5 - down.shape[0], 5)]
        sets = [(up, below), (down, above)]
    partial = attend(where, turned, starts, sets, state, weight)

    other = lax.ppermute(partial[1], "head", [(h, h ^ 1) for h in range(8)])
    both = (partial[0].astype(jnp.float32) + other.astype(jnp.float32)).astype(jnp.bfloat16)
    parts = lax.all_to_all(
        both, "head", 0, 0, axis_index_groups=[[0, 2, 4, 6], [1, 3, 5, 7]], tiled=True
    )
    return jnp.sum(parts.astype(jnp.float32), axis=0).astype(jnp.bfloat16)


def solution(mesh):
    placed = (
        P("seq", "head", None),
        P("seq", "head", None),
        P("seq", "head", None),
        P("head", "seq"),
        P(),
    )
    return jax.shard_map(layer, mesh=mesh, in_specs=placed, out_specs=P("seq", "head"), check_vma=False)
```

```python
import math

import jax
import jax.numpy as jnp
from jax import lax
from jax.experimental import pallas as pl
from jax.experimental.pallas import tpu as pltpu
from jax.sharding import PartitionSpec as P


NEG = -1e30
WIDE = 4


def visit(where_ref, q_ref, starts_ref, block_ref, nearest, accum, top):
    heads, tok, width = q_ref.shape
    factor = math.log2(math.e) / math.sqrt(width)
    count = block_ref.shape[0]
    me, first, last_start = where_ref[0], where_ref[1], where_ref[2]

    def add(keys, vals, allowed):
        vals = jnp.concatenate([vals, jnp.ones(vals.shape, jnp.bfloat16)], axis=1)
        for h in range(heads):
            scores = lax.dot_general(
                q_ref[h], keys, (((1,), (1,)), ((), ())), preferred_element_type=jnp.float32
            )
            if allowed is not None:
                scores = jnp.where(allowed, scores, NEG)
            old = top[h][:, :1]
            new = jnp.maximum(old, jnp.max(scores, axis=1, keepdims=True))
            weights = jnp.exp2((scores - new) * factor).astype(jnp.bfloat16)
            rescale = jnp.exp2((old - new) * factor)
            accum[h] = accum[h] * rescale + jnp.dot(weights, vals, preferred_element_type=jnp.float32)
            top[h] = jnp.broadcast_to(new, (tok, width))

    begin = 0
    if nearest < 0 and count >= WIDE:
        full = (me + nearest - 8 * (WIDE - 1)) * tok >= last_start
        begin = jnp.where(full, WIDE, 0)

        @pl.when(full)
        def _():
            span = WIDE * tok
            keys = block_ref[:WIDE, :tok, :].reshape(span, width)
            add(keys, block_ref[:WIDE, tok:, :].reshape(span, width), None)

    @pl.loop(begin, count)
    def _(k):
        place = me + nearest - 8 * k

        @pl.when((place >= first) & (place >= 0))
        def _():
            key_pos = place * tok + lax.broadcasted_iota(jnp.int32, (1, tok), 1)
            query_pos = me * tok + lax.broadcasted_iota(jnp.int32, (tok, 1), 0)
            allowed = (key_pos >= starts_ref[:, :1]) & (key_pos <= query_pos)
            block = block_ref[k]
            add(block[:tok], block[tok:], allowed)


def attend(where, queries, starts, sets, state, weights=None):
    heads, tok, width = queries.shape
    arrays = [array for array, _ in sets]
    count = len(sets)
    state_shapes = [
        jax.ShapeDtypeStruct((heads, tok, 2 * width), jnp.float32),
        jax.ShapeDtypeStruct((heads, tok, width), jnp.float32),
    ]
    vmem = pl.BlockSpec(memory_space=pltpu.VMEM)
    specs = [pl.BlockSpec(memory_space=pltpu.SMEM)] + [vmem] * (2 + count)
    keys_seen = sum(array.shape[0] for array in arrays) * tok
    cost = pl.CostEstimate(
        flops=4 * heads * tok * keys_seen * width,
        bytes_accessed=4 * keys_seen * width,
        transcendentals=heads * tok * keys_seen,
    )
    limit = pltpu.CompilerParams(vmem_limit_bytes=32 * 1024 * 1024)

    def visit_all(where_ref, q_ref, starts_ref, blocks, accum, top):
        for block, (_, nearest) in zip(blocks, sets):
            visit(where_ref, q_ref, starts_ref, block, nearest, accum, top)

    if weights is None:

        def kernel(where_ref, q_ref, starts_ref, *refs):
            accum, top = refs[-2:]
            if state is None:
                accum[...] = jnp.zeros_like(accum)
                top[...] = jnp.full_like(top, NEG)
            visit_all(where_ref, q_ref, starts_ref, refs[:count], accum, top)

        given = [] if state is None else list(state)
        return pl.pallas_call(
            kernel,
            out_shape=state_shapes,
            in_specs=specs + [vmem] * len(given),
            out_specs=[vmem, vmem],
            input_output_aliases={} if state is None else {3 + count: 0, 4 + count: 1},
            compiler_params=limit,
            cost_estimate=cost,
            name="attend",
        )(where, queries, starts, *arrays, *given)

    cols = weights[0][0].shape[0]

    def last(where_ref, q_ref, starts_ref, *refs):
        accum_in, top_in, *weight_refs = refs[count:-3]
        out_ref, accum, top = refs[-3:]
        accum[...] = accum_in[...]
        top[...] = top_in[...]
        visit_all(where_ref, q_ref, starts_ref, refs[:count], accum, top)
        attended = jnp.concatenate(
            [(accum[h][:, :width] / accum[h][:, width:]).astype(jnp.bfloat16) for h in range(heads)], axis=1
        )
        core, plane = where_ref[3], where_ref[4]
        for weight_ref, (_, distance) in zip(weight_refs, weights):
            owner = lax.rem(plane + 8 - distance, 8)
            sent = jnp.bitwise_xor(owner & 1, core)
            out_ref[sent, owner >> 1] = lax.dot_general(
                attended, weight_ref[...], (((1,), (1,)), ((), ())), preferred_element_type=jnp.float32
            ).astype(jnp.bfloat16)

    return pl.pallas_call(
        last,
        out_shape=jax.ShapeDtypeStruct((2, 4, tok, cols), jnp.bfloat16),
        in_specs=specs + [vmem] * (2 + len(weights)),
        out_specs=vmem,
        scratch_shapes=[pltpu.VMEM(shape.shape, jnp.float32) for shape in state_shapes],
        compiler_params=limit,
        cost_estimate=cost,
        name="finish",
    )(where, queries, starts, *arrays, *state, *[weight for weight, _ in weights])


def moved(array, steps):
    count = lax.axis_size("seq")
    return lax.ppermute(array, "seq", [(i, (i + steps) % count) for i in range(count)])


def layer(queries, keys, values, out_weight, doc_lengths):
    tok, _, width = queries.shape
    me = lax.axis_index("seq")
    core = lax.axis_index("head") % 2

    own = jnp.concatenate([keys.reshape(1, tok, width), values.reshape(1, tok, width)], axis=1)
    near = moved(own, 8)
    far = moved(own, 32)
    two = jnp.concatenate([own, near], axis=0)
    double = moved(two, 16)
    turned = out_weight.T
    weight = lax.all_to_all(
        jnp.broadcast_to(turned[None], (8,) + turned.shape),
        "seq",
        0,
        0,
        axis_index_groups=[[8 * z + y for y in range(8)] for z in range(8)],
        tiled=True,
    ).reshape(8 * turned.shape[0], turned.shape[1])
    column = jnp.concatenate([two, double, far], axis=0)

    ends = jnp.cumsum(doc_lengths)
    position = me * tok + jnp.arange(tok, dtype=jnp.int32)
    starts = jnp.max(jnp.where(ends[None, :] <= position[:, None], ends[None, :], 0), axis=1)
    where = jnp.stack([me, starts[0] // tok, starts[-1], core, me // 8]).astype(jnp.int32)
    starts = jnp.broadcast_to(starts[:, None], (tok, 128))
    queries = jnp.transpose(queries, (1, 0, 2))

    weights = [(weight, 0)]
    ahead = behind = weight
    sets, state = [(column, 0)], None
    up, down = column, column[1:]
    for turn in range(1, 5):
        up = moved(up if turn == 1 else up[:4] if turn < 4 else up[:2], 1)
        down = moved(down if turn < 4 else down[2:], -1)
        ahead = moved(ahead, 8)
        weights.append((ahead, turn))
        if turn < 4:
            behind = moved(behind, -8)
            weights.append((behind, 8 - turn))
        state = attend(where, queries, starts, sets, state)
        sets = [(up, -turn), (down, turn - 8 * (5 - down.shape[0]))]
    partial = attend(where, queries, starts, sets, state, weights)

    other = lax.ppermute(partial[1], "head", [(h, h ^ 1) for h in range(8)])
    both = (partial[0].astype(jnp.float32) + other.astype(jnp.float32)).astype(jnp.bfloat16)
    parts = lax.all_to_all(
        both, "head", 0, 0, axis_index_groups=[[0, 2, 4, 6], [1, 3, 5, 7]], tiled=True
    )
    return jnp.sum(parts.astype(jnp.float32), axis=0).astype(jnp.bfloat16)


def solution(mesh):
    placed = (
        P("seq", "head", None),
        P("seq", "head", None),
        P("seq", "head", None),
        P("head", "seq"),
        P(),
    )
    return jax.shard_map(layer, mesh=mesh, in_specs=placed, out_specs=P("seq", "head"), check_vma=False)
```

```python
import math

import jax
import jax.numpy as jnp
from jax import lax
from jax.experimental import pallas as pl
from jax.experimental.pallas import tpu as pltpu
from jax.sharding import PartitionSpec as P


NEG = -1e30


def visit(where_ref, q_ref, starts_ref, blocks, accum, top):
    heads, tok, width = q_ref.shape
    factor = math.log2(math.e) / math.sqrt(width)
    me, first = where_ref[0], where_ref[1]

    def add(chosen):
        keys = jnp.concatenate([ref[k, :tok, :] for ref, k, _ in chosen], axis=0)
        vals = jnp.concatenate([ref[k, tok:, :] for ref, k, _ in chosen], axis=0)
        vals = jnp.concatenate([vals, jnp.ones(vals.shape, jnp.bfloat16)], axis=1)
        lane = lax.broadcasted_iota(jnp.int32, (1, tok), 1)
        key_pos = jnp.concatenate([lane + (me + offset) * tok for _, _, offset in chosen], axis=1)
        allowed = key_pos >= starts_ref[:, :1]
        if chosen[0][2] == 0:
            allowed &= key_pos <= me * tok + lax.broadcasted_iota(jnp.int32, (tok, 1), 0)
        for h in range(heads):
            scores = lax.dot_general(
                q_ref[h], keys, (((1,), (1,)), ((), ())), preferred_element_type=jnp.float32
            )
            scores = jnp.where(allowed, scores, NEG)
            old = top[h][:, :1]
            new = jnp.maximum(old, jnp.max(scores, axis=1, keepdims=True))
            weights = jnp.exp2((scores - new) * factor).astype(jnp.bfloat16)
            rescale = jnp.exp2((old - new) * factor)
            accum[h] = accum[h] * rescale + jnp.dot(weights, vals, preferred_element_type=jnp.float32)
            top[h] = jnp.broadcast_to(new, (tok, width))

    pl.when(me + blocks[0][2] >= first)(lambda: add(blocks))


def attend(where, queries, starts, sets, state, finish=False):
    heads, tok, width = queries.shape
    arrays = [array for array, _, _ in sets]
    count = len(sets)
    state_shapes = [
        jax.ShapeDtypeStruct((heads, tok, 2 * width), jnp.float32),
        jax.ShapeDtypeStruct((heads, tok, width), jnp.float32),
    ]
    out_shape = state_shapes
    if finish:
        out_shape = [jax.ShapeDtypeStruct((4, tok, heads * width), jnp.bfloat16)]
    vmem = pl.BlockSpec(memory_space=pltpu.VMEM)
    given = [] if state is None else list(state)
    keys_seen = sum(array.shape[0] for array in arrays) * tok

    def kernel(where_ref, q_ref, starts_ref, *refs):
        if finish:
            accum_in, top_in, out_ref, accum, top = refs[count:]
            accum[...] = accum_in[...]
            top[...] = top_in[...]
        else:
            accum, top = refs[-2:]
        if state is None:
            accum[...] = jnp.zeros_like(accum)
            top[...] = jnp.full_like(top, NEG)
        groups = {}
        for ref, (_, group, offsets) in zip(refs, sets):
            groups.setdefault(group, []).extend((ref, k, offset) for k, offset in enumerate(offsets))
        for blocks in groups.values():
            visit(where_ref, q_ref, starts_ref, blocks, accum, top)
        if finish:
            for h in range(heads):
                attended = (accum[h][:, :width] / accum[h][:, width:]).astype(jnp.bfloat16)
                for copy in range(4):
                    out_ref[copy, :, h * width : (h + 1) * width] = attended

    return pl.pallas_call(
        kernel,
        out_shape=out_shape,
        in_specs=[pl.BlockSpec(memory_space=pltpu.SMEM)] + [vmem] * (2 + count + len(given)),
        out_specs=[vmem] * len(out_shape),
        input_output_aliases={} if finish or state is None else {3 + count: 0, 4 + count: 1},
        scratch_shapes=[pltpu.VMEM(shape.shape, jnp.float32) for shape in state_shapes] if finish else [],
        compiler_params=pltpu.CompilerParams(vmem_limit_bytes=32 * 1024 * 1024),
        cost_estimate=pl.CostEstimate(
            flops=4 * heads * tok * keys_seen * width,
            bytes_accessed=4 * keys_seen * width,
            transcendentals=heads * tok * keys_seen,
        ),
        name="attend",
    )(where, queries, starts, *arrays, *given)


def project(where, mine, others, weight):
    groups, cols, _ = weight.shape
    tok = mine.shape[1]

    def kernel(where_ref, mine_ref, others_ref, weight_ref, out_ref, held, sems):
        copies = [
            pltpu.make_async_copy(weight_ref.at[group], held.at[group], sems.at[group]) for group in range(groups)
        ]
        for copy in copies:
            copy.start()
        core = where_ref[3]
        total = jnp.zeros((tok, cols), jnp.float32)
        for group in range(groups):
            rows = jnp.where(core == group % 2, mine_ref[group // 2], others_ref[group // 2])
            copies[group].wait()
            total += lax.dot_general(
                rows, held[group], (((1,), (1,)), ((), ())), preferred_element_type=jnp.float32
            )
        out_ref[...] = total.astype(jnp.bfloat16)

    vmem = pl.BlockSpec(memory_space=pltpu.VMEM)
    return pl.pallas_call(
        kernel,
        out_shape=jax.ShapeDtypeStruct((tok, cols), jnp.bfloat16),
        in_specs=[pl.BlockSpec(memory_space=pltpu.SMEM), vmem, vmem, pl.BlockSpec(memory_space=pltpu.HBM)],
        out_specs=vmem,
        scratch_shapes=[pltpu.VMEM(weight.shape, jnp.bfloat16), pltpu.SemaphoreType.DMA((groups,))],
        compiler_params=pltpu.CompilerParams(vmem_limit_bytes=32 * 1024 * 1024),
        name="project",
    )(where, mine, others, pltpu.with_memory_space_constraint(weight, pltpu.HBM))


def moved(array, steps):
    count = lax.axis_size("seq")
    return lax.ppermute(array, "seq", [(i, (i + steps) % count) for i in range(count)])


def layer(queries, keys, values, out_weight, doc_lengths):
    tok, _, width = queries.shape
    me = lax.axis_index("seq")
    core = lax.axis_index("head") % 2

    own = jnp.concatenate([keys.reshape(1, tok, width), values.reshape(1, tok, width)], axis=1)
    near = moved(own, 8)
    two = jnp.concatenate([own, near], axis=0)
    double = moved(two, 16)
    column = jnp.concatenate([two, double], axis=0)
    places = [(z, y, h) for z in range(8) for y in range(8) for h in range(8)]
    block = lax.ppermute(
        out_weight.T,
        ("seq", "head"),
        [(64 * z + 8 * y + h, 64 * h + 8 * y + z) for z, y, h in places],
    )
    weight = lax.all_gather(block, "seq", axis=0, tiled=True).reshape(8, -1, block.shape[1])

    ends = jnp.cumsum(doc_lengths)
    position = me * tok + jnp.arange(tok, dtype=jnp.int32)
    starts = jnp.max(jnp.where(ends[None, :] <= position[:, None], ends[None, :], 0), axis=1)
    where = jnp.stack([me, starts[0] // tok, starts[-1], core]).astype(jnp.int32)
    starts = jnp.broadcast_to(starts[:, None], (tok, 128))
    queries = jnp.transpose(queries, (1, 0, 2))

    sets, state = [(column, 0, [0, -8, -16, -24])], None
    up = down = column
    for turn in range(1, 6):
        if turn < 5:
            up = moved(up if turn < 4 else up[:2], 1)
            down = moved(down, 7) if turn == 1 else moved(down if turn < 4 else down[2:], -1)
        if turn == 1:
            edge = jnp.concatenate([column[3:], up[3:]], axis=0)
        if turn == 2:
            edge = moved(edge, 8)
        state = attend(where, queries, starts, sets, state, turn == 5)
        below = [-turn - 8 * a for a in range(4)]
        above = [turn - 8 - 8 * a for a in range(4)]
        if turn < 4:
            sets = [(up, 0, below), (down, 1, above)]
        else:
            sets = [(up, 0, below[:2]), (down, 0, above[2:]), (edge, 1, [-32, -33])]

    mine = lax.all_to_all(
        state[0], "head", 0, 0, axis_index_groups=[[0, 2, 4, 6], [1, 3, 5, 7]], tiled=True
    )
    others = lax.ppermute(mine, "head", [(h, h ^ 1) for h in range(8)])
    return project(where, mine, others, weight)


def solution(mesh):
    placed = (
        P("seq", "head", None),
        P("seq", "head", None),
        P("seq", "head", None),
        P("head", "seq"),
        P(),
    )
    return jax.shard_map(layer, mesh=mesh, in_specs=placed, out_specs=P("seq", "head"), check_vma=False)
```

```python
import math

import jax
import jax.numpy as jnp
from jax import lax
from jax.experimental import pallas as pl
from jax.experimental.pallas import tpu as pltpu
from jax.sharding import PartitionSpec as P


NEG = -1e30


def visit(where_ref, q_ref, starts_ref, blocks, nearest, accum, top, causal=False):
    heads, tok, width = q_ref.shape
    factor = math.log2(math.e) / math.sqrt(width)
    me, first = where_ref[0], where_ref[1]

    def add():
        keys = jnp.concatenate([ref[k, :tok, :] for ref, k, _ in blocks], axis=0)
        vals = jnp.concatenate([ref[k, tok:, :] for ref, k, _ in blocks], axis=0)
        vals = jnp.concatenate([vals, jnp.ones(vals.shape, jnp.bfloat16)], axis=1)
        lane = lax.broadcasted_iota(jnp.int32, (1, tok), 1)
        key_pos = jnp.concatenate([lane + number * tok for _, _, number in blocks], axis=1)
        allowed = key_pos >= starts_ref[:, :1]
        if causal:
            allowed &= key_pos <= me * tok + lax.broadcasted_iota(jnp.int32, (tok, 1), 0)
        for h in range(heads):
            scores = lax.dot_general(
                q_ref[h], keys, (((1,), (1,)), ((), ())), preferred_element_type=jnp.float32
            )
            scores = jnp.where(allowed, scores, NEG)
            old = top[h][:, :1]
            new = jnp.maximum(old, jnp.max(scores, axis=1, keepdims=True))
            weights = jnp.exp2((scores - new) * factor).astype(jnp.bfloat16)
            rescale = jnp.exp2((old - new) * factor)
            accum[h] = accum[h] * rescale + jnp.dot(weights, vals, preferred_element_type=jnp.float32)
            top[h] = jnp.broadcast_to(new, (tok, width))

    pl.when(me + nearest >= first)(add)


def attend(where, queries, starts, arrays, plan, state, finish=False):
    heads, tok, width = queries.shape
    count = len(arrays)
    state_shapes = [
        jax.ShapeDtypeStruct((heads, tok, 2 * width), jnp.float32),
        jax.ShapeDtypeStruct((heads, tok, width), jnp.float32),
    ]
    out_shape = state_shapes
    if finish:
        out_shape = [jax.ShapeDtypeStruct((tok, heads * width), jnp.bfloat16)]
    vmem = pl.BlockSpec(memory_space=pltpu.VMEM)
    given = [] if state is None else list(state)
    keys_seen = 8 * tok

    def kernel(where_ref, q_ref, starts_ref, *refs):
        if finish:
            accum_in, top_in, out_ref, accum, top = refs[count:]
            accum[...] = accum_in[...]
            top[...] = top_in[...]
        else:
            accum, top = refs[-2:]
        if state is None:
            accum[...] = jnp.zeros_like(accum)
            top[...] = jnp.full_like(top, NEG)
        for blocks, nearest, causal in plan(where_ref, refs[:count]):
            visit(where_ref, q_ref, starts_ref, blocks, nearest, accum, top, causal)
        if finish:
            for h in range(heads):
                out_ref[:, h * width : (h + 1) * width] = (
                    accum[h][:, :width] / accum[h][:, width:]
                ).astype(jnp.bfloat16)

    return pl.pallas_call(
        kernel,
        out_shape=out_shape,
        in_specs=[pl.BlockSpec(memory_space=pltpu.SMEM)] + [vmem] * (2 + count + len(given)),
        out_specs=[vmem] * len(out_shape),
        input_output_aliases={} if finish or state is None else {3 + count: 0, 4 + count: 1},
        scratch_shapes=[pltpu.VMEM(shape.shape, jnp.float32) for shape in state_shapes] if finish else [],
        compiler_params=pltpu.CompilerParams(vmem_limit_bytes=16 * 1024 * 1024),
        cost_estimate=pl.CostEstimate(
            flops=4 * heads * tok * keys_seen * width,
            bytes_accessed=4 * keys_seen * width,
            transcendentals=heads * tok * keys_seen,
        ),
        name="attend",
    )(where, queries, starts, *arrays, *given)


def project(where, attended, weight):
    tok, depth = attended.shape
    groups = 8
    weight = weight.reshape(groups, -1, depth)
    cols = weight.shape[1]

    def kernel(where_ref, attended_ref, weight_ref, out_ref, held, sems):
        copies = [
            pltpu.make_async_copy(weight_ref.at[group], held.at[group], sems.at[group]) for group in range(groups)
        ]
        for copy in copies:
            copy.start()
        core = where_ref[3]
        for group in range(groups):
            copies[group].wait()
            sent = jnp.bitwise_xor(core, group % 2)
            out_ref[sent, group // 2] = lax.dot_general(
                attended_ref[...], held[group], (((1,), (1,)), ((), ())), preferred_element_type=jnp.float32
            ).astype(jnp.bfloat16)

    vmem = pl.BlockSpec(memory_space=pltpu.VMEM)
    return pl.pallas_call(
        kernel,
        out_shape=jax.ShapeDtypeStruct((2, groups // 2, tok, cols), jnp.bfloat16),
        in_specs=[pl.BlockSpec(memory_space=pltpu.SMEM), vmem, pl.BlockSpec(memory_space=pltpu.HBM)],
        out_specs=vmem,
        scratch_shapes=[pltpu.VMEM(weight.shape, jnp.bfloat16), pltpu.SemaphoreType.DMA((groups,))],
        compiler_params=pltpu.CompilerParams(vmem_limit_bytes=16 * 1024 * 1024),
        name="project",
    )(where, attended, pltpu.with_memory_space_constraint(weight, pltpu.HBM))


def down_column(array, steps):
    return lax.ppermute(
        array, "seq", [(8 * z + y, 8 * ((z + steps) % 8) + y) for z in range(8) for y in range(8)]
    )


def along_row(array, steps):
    return lax.ppermute(
        array, "seq", [(8 * z + y, 8 * z + (y + steps) % 8) for z in range(8) for y in range(8)]
    )


def layer(queries, keys, values, out_weight, doc_lengths):
    tok, _, width = queries.shape
    me = lax.axis_index("seq")
    core = lax.axis_index("head") % 2

    own = jnp.concatenate([keys.reshape(1, tok, width), values.reshape(1, tok, width)], axis=1)
    near = down_column(own, 1)
    far = down_column(own, 4)
    two = jnp.concatenate([own, near], axis=0)
    double = down_column(two, 2)
    column = jnp.concatenate([two, double, far], axis=0)
    turned = out_weight.T
    weight = lax.all_to_all(
        jnp.broadcast_to(turned[None], (8,) + turned.shape),
        "seq",
        0,
        0,
        axis_index_groups=[[8 * z + y for y in range(8)] for z in range(8)],
        tiled=True,
    ).reshape(8 * turned.shape[0], turned.shape[1])
    weight = lax.all_gather(
        weight,
        "seq",
        axis=0,
        axis_index_groups=[[8 * z + y for z in range(8)] for y in range(8)],
        tiled=True,
    )

    ends = jnp.cumsum(doc_lengths)
    position = me * tok + jnp.arange(tok, dtype=jnp.int32)
    starts = jnp.max(jnp.where(ends[None, :] <= position[:, None], ends[None, :], 0), axis=1)
    where = jnp.stack([me, starts[0] // tok, starts[-1], core, me % 8]).astype(jnp.int32)
    starts = jnp.broadcast_to(starts[:, None], (tok, 128))
    queries = jnp.transpose(queries, (1, 0, 2))


    def own_plan(where_ref, refs):
        me = where_ref[0]
        yield [(refs[0], a, me - 8 * a) for a in range(4)], 0, True

    def turn_plan(turn):
        def plan(where_ref, refs):
            me, place = where_ref[0], where_ref[4]
            skip = jnp.where(place >= turn, 0, 1)
            yield [(refs[0], skip + a, me - turn - 8 * a) for a in range(4)], -turn, False
            skip = jnp.where(place + turn < 8, 1, 0)
            yield [(refs[1], skip + a, me + turn - 8 - 8 * a) for a in range(4)], turn - 8, False

        return plan

    def last_plan(where_ref, refs):
        me, place = where_ref[0], where_ref[4]
        up, down, column, first_up, edge = refs
        shift = jnp.where(place >= 4, -4, 4)
        numbers = [me + shift - 8 * a for a in range(5)]
        numbers = [jnp.where(number > me, -1, number) for number in numbers]
        blocks = [(up, a, numbers[a]) for a in range(3)] + [(down, a, numbers[3 + a]) for a in range(2)]
        yield blocks, -4, False
        yield [(column, 4, me - 32)], -32, False
        beyond = jnp.where(place > 0, me - 33, -1)
        blocks = [(first_up, 4, beyond), (edge, 0, jnp.where(place > 0, -1, me - 33))]
        yield blocks, -33, False

    state, arrays, plan = None, [column], own_plan
    up = down = column
    for turn in range(1, 5):
        up = along_row(up if turn < 4 else up[:3], 1)
        down = along_row(down if turn < 4 else down[3:], -1)
        if turn == 1:
            first_up = up
        state = attend(where, queries, starts, arrays, plan, state)
        arrays, plan = [up, down], turn_plan(turn)
    edge = lax.ppermute(column[:1], "seq", [(8 * z + 7, 8 * ((z + 5) % 8)) for z in range(8)])
    arrays = [up, down, column, first_up, edge]
    (attended,) = attend(where, queries, starts, arrays, last_plan, state, True)
    partial = project(where, attended, weight)

    other = lax.ppermute(partial[1], "head", [(h, h ^ 1) for h in range(8)])
    both = (partial[0].astype(jnp.float32) + other.astype(jnp.float32)).astype(jnp.bfloat16)
    parts = lax.all_to_all(
        both, "head", 0, 0, axis_index_groups=[[0, 2, 4, 6], [1, 3, 5, 7]], tiled=True
    )
    return jnp.sum(parts.astype(jnp.float32), axis=0).astype(jnp.bfloat16)


def solution(mesh):
    placed = (
        P("seq", "head", None),
        P("seq", "head", None),
        P("seq", "head", None),
        P("head", "seq"),
        P(),
    )
    return jax.shard_map(layer, mesh=mesh, in_specs=placed, out_specs=P("seq", "head"), check_vma=False)
```

```python
import math

import jax
import jax.numpy as jnp
from jax import lax
from jax.experimental import pallas as pl
from jax.experimental.pallas import tpu as pltpu
from jax.sharding import PartitionSpec as P


NEG = -1e30


def visit(where_ref, q_ref, starts_ref, blocks, nearest, accum, top, causal=False):
    heads, tok, width = q_ref.shape
    factor = math.log2(math.e) / math.sqrt(width)
    me, first = where_ref[0], where_ref[1]

    def add():
        keys = jnp.concatenate([ref[k, :tok, :] for ref, k, _ in blocks], axis=0)
        vals = jnp.concatenate([ref[k, tok:, :] for ref, k, _ in blocks], axis=0)
        vals = jnp.concatenate([vals, jnp.ones(vals.shape, jnp.bfloat16)], axis=1)
        lane = lax.broadcasted_iota(jnp.int32, (1, tok), 1)
        key_pos = jnp.concatenate([lane + number * tok for _, _, number in blocks], axis=1)
        allowed = key_pos >= starts_ref[:, :1]
        if causal:
            allowed &= key_pos <= me * tok + lax.broadcasted_iota(jnp.int32, (tok, 1), 0)
        for h in range(heads):
            scores = lax.dot_general(
                q_ref[h], keys, (((1,), (1,)), ((), ())), preferred_element_type=jnp.float32
            )
            scores = jnp.where(allowed, scores, NEG)
            old = top[h][:, :1]
            new = jnp.maximum(old, jnp.max(scores, axis=1, keepdims=True))
            weights = jnp.exp2((scores - new) * factor).astype(jnp.bfloat16)
            rescale = jnp.exp2((old - new) * factor)
            accum[h] = accum[h] * rescale + jnp.dot(weights, vals, preferred_element_type=jnp.float32)
            top[h] = jnp.broadcast_to(new, (tok, width))

    pl.when(me + nearest >= first)(add)


def attend(where, queries, starts, arrays, plan, state, finish=False):
    heads, tok, width = queries.shape
    count = len(arrays)
    state_shapes = [
        jax.ShapeDtypeStruct((heads, tok, 2 * width), jnp.float32),
        jax.ShapeDtypeStruct((heads, tok, width), jnp.float32),
    ]
    out_shape = state_shapes
    if finish:
        out_shape = [jax.ShapeDtypeStruct((tok, heads * width), jnp.bfloat16)]
    vmem = pl.BlockSpec(memory_space=pltpu.VMEM)
    given = [] if state is None else list(state)
    keys_seen = 8 * tok

    def kernel(where_ref, q_ref, starts_ref, *refs):
        if finish:
            accum_in, top_in, out_ref, accum, top = refs[count:]
            accum[...] = accum_in[...]
            top[...] = top_in[...]
        else:
            accum, top = refs[-2:]
        if state is None:
            accum[...] = jnp.zeros_like(accum)
            top[...] = jnp.full_like(top, NEG)
        for blocks, nearest, causal in plan(where_ref, refs[:count]):
            visit(where_ref, q_ref, starts_ref, blocks, nearest, accum, top, causal)
        if finish:
            for h in range(heads):
                out_ref[:, h * width : (h + 1) * width] = (
                    accum[h][:, :width] / accum[h][:, width:]
                ).astype(jnp.bfloat16)

    return pl.pallas_call(
        kernel,
        out_shape=out_shape,
        in_specs=[pl.BlockSpec(memory_space=pltpu.SMEM)] + [vmem] * (2 + count + len(given)),
        out_specs=[vmem] * len(out_shape),
        input_output_aliases={} if finish or state is None else {3 + count: 0, 4 + count: 1},
        scratch_shapes=[pltpu.VMEM(shape.shape, jnp.float32) for shape in state_shapes] if finish else [],
        compiler_params=pltpu.CompilerParams(vmem_limit_bytes=16 * 1024 * 1024),
        cost_estimate=pl.CostEstimate(
            flops=4 * heads * tok * keys_seen * width,
            bytes_accessed=4 * keys_seen * width,
            transcendentals=heads * tok * keys_seen,
        ),
        name="attend",
    )(where, queries, starts, *arrays, *given)


def project(where, attended, weights):
    tok, _ = attended.shape
    cols = weights[0][0].shape[0]

    def kernel(where_ref, attended_ref, *refs):
        *weight_refs, out_ref = refs
        core, plane = where_ref[3], where_ref[0] // 8
        for weight_ref, (_, distance) in zip(weight_refs, weights):
            owner = lax.rem(plane + 8 - distance, 8)
            out_ref[jnp.bitwise_xor(owner & 1, core), owner >> 1] = lax.dot_general(
                attended_ref[...], weight_ref[...], (((1,), (1,)), ((), ())), preferred_element_type=jnp.float32
            ).astype(jnp.bfloat16)

    vmem = pl.BlockSpec(memory_space=pltpu.VMEM)
    return pl.pallas_call(
        kernel,
        out_shape=jax.ShapeDtypeStruct((2, 4, tok, cols), jnp.bfloat16),
        in_specs=[pl.BlockSpec(memory_space=pltpu.SMEM)] + [vmem] * (1 + len(weights)),
        out_specs=vmem,
        compiler_params=pltpu.CompilerParams(vmem_limit_bytes=16 * 1024 * 1024),
        name="project",
    )(where, attended, *[weight for weight, _ in weights])


def down_column(array, steps):
    return lax.ppermute(
        array, "seq", [(8 * z + y, 8 * ((z + steps) % 8) + y) for z in range(8) for y in range(8)]
    )


def along_row(array, steps):
    return lax.ppermute(
        array, "seq", [(8 * z + y, 8 * z + (y + steps) % 8) for z in range(8) for y in range(8)]
    )


def layer(queries, keys, values, out_weight, doc_lengths):
    tok, _, width = queries.shape
    me = lax.axis_index("seq")
    core = lax.axis_index("head") % 2

    own = jnp.concatenate([keys.reshape(1, tok, width), values.reshape(1, tok, width)], axis=1)
    near = down_column(own, 1)
    far = down_column(own, 4)
    two = jnp.concatenate([own, near], axis=0)
    double = down_column(two, 2)
    column = jnp.concatenate([two, double, far], axis=0)
    turned = out_weight.T
    weight = lax.all_to_all(
        jnp.broadcast_to(turned[None], (8,) + turned.shape),
        "seq",
        0,
        0,
        axis_index_groups=[[8 * z + y for y in range(8)] for z in range(8)],
        tiled=True,
    ).reshape(8 * turned.shape[0], turned.shape[1])
    ends = jnp.cumsum(doc_lengths)
    position = me * tok + jnp.arange(tok, dtype=jnp.int32)
    starts = jnp.max(jnp.where(ends[None, :] <= position[:, None], ends[None, :], 0), axis=1)
    where = jnp.stack([me, starts[0] // tok, starts[-1], core, me % 8]).astype(jnp.int32)
    starts = jnp.broadcast_to(starts[:, None], (tok, 128))
    queries = jnp.transpose(queries, (1, 0, 2))


    def own_plan(where_ref, refs):
        me = where_ref[0]
        yield [(refs[0], a, me - 8 * a) for a in range(4)], 0, True

    def turn_plan(turn):
        def plan(where_ref, refs):
            me, place = where_ref[0], where_ref[4]
            skip = jnp.where(place >= turn, 0, 1)
            yield [(refs[0], skip + a, me - turn - 8 * a) for a in range(4)], -turn, False
            skip = jnp.where(place + turn < 8, 1, 0)
            yield [(refs[1], skip + a, me + turn - 8 - 8 * a) for a in range(4)], turn - 8, False

        return plan

    def last_plan(where_ref, refs):
        me, place = where_ref[0], where_ref[4]
        up, down, column, first_up, edge = refs
        shift = jnp.where(place >= 4, -4, 4)
        numbers = [me + shift - 8 * a for a in range(5)]
        numbers = [jnp.where(number > me, -1, number) for number in numbers]
        blocks = [(up, a, numbers[a]) for a in range(3)] + [(down, a, numbers[3 + a]) for a in range(2)]
        yield blocks, -4, False
        beyond = jnp.where(place > 0, me - 33, -1)
        blocks = [(column, 4, me - 32), (first_up, 4, beyond), (edge, 0, jnp.where(place > 0, -1, me - 33))]
        yield blocks, -32, False

    state, arrays, plan = None, [column], own_plan
    up = down = column
    ahead = behind = weight
    weights = [(weight, 0)]
    for turn in range(1, 5):
        up = along_row(up if turn < 4 else up[:3], 1)
        down = along_row(down if turn < 4 else down[3:], -1)
        if turn == 1:
            first_up = up
        state = attend(where, queries, starts, arrays, plan, state)
        behind = down_column(behind, -1)
        weights.append((behind, 8 - turn))
        if turn < 4:
            ahead = down_column(ahead, 1)
            weights.append((ahead, turn))
        arrays, plan = [up, down], turn_plan(turn)
    edge = lax.ppermute(column[:1], "seq", [(8 * z + 7, 8 * ((z + 5) % 8)) for z in range(8)])
    arrays = [up, down, column, first_up, edge]
    (attended,) = attend(where, queries, starts, arrays, last_plan, state, True)
    partial = project(where, attended, weights)

    other = lax.ppermute(partial[1], "head", [(h, h ^ 1) for h in range(8)])
    both = (partial[0].astype(jnp.float32) + other.astype(jnp.float32)).astype(jnp.bfloat16)
    parts = lax.all_to_all(
        both, "head", 0, 0, axis_index_groups=[[0, 2, 4, 6], [1, 3, 5, 7]], tiled=True
    )
    return jnp.sum(parts.astype(jnp.float32), axis=0).astype(jnp.bfloat16)


def solution(mesh):
    placed = (
        P("seq", "head", None),
        P("seq", "head", None),
        P("seq", "head", None),
        P("head", "seq"),
        P(),
    )
    return jax.shard_map(layer, mesh=mesh, in_specs=placed, out_specs=P("seq", "head"), check_vma=False)
```

```python
import math

import jax
import jax.numpy as jnp
from jax import lax
from jax.experimental import pallas as pl
from jax.experimental.pallas import tpu as pltpu
from jax.sharding import PartitionSpec as P


NEG = -1e30


def visit(where_ref, q_ref, starts_ref, blocks, nearest, accum, top, causal=False):
    heads, tok, width = q_ref.shape
    factor = math.log2(math.e) / math.sqrt(width)
    me, first = where_ref[0], where_ref[1]

    def add():
        keys = jnp.concatenate([ref[k, :tok, :] for ref, k, _ in blocks], axis=0)
        vals = jnp.concatenate([ref[k, tok:, :] for ref, k, _ in blocks], axis=0)
        vals = jnp.concatenate([vals, jnp.ones(vals.shape, jnp.bfloat16)], axis=1)
        lane = lax.broadcasted_iota(jnp.int32, (1, tok), 1)
        key_pos = jnp.concatenate([lane + number * tok for _, _, number in blocks], axis=1)
        allowed = key_pos >= starts_ref[:, :1]
        if causal:
            allowed &= key_pos <= me * tok + lax.broadcasted_iota(jnp.int32, (tok, 1), 0)
        for h in range(heads):
            scores = lax.dot_general(
                q_ref[h], keys, (((1,), (1,)), ((), ())), preferred_element_type=jnp.float32
            )
            scores = jnp.where(allowed, scores, NEG)
            old = top[h][:, :1]
            new = jnp.maximum(old, jnp.max(scores, axis=1, keepdims=True))
            weights = jnp.exp2((scores - new) * factor).astype(jnp.bfloat16)
            rescale = jnp.exp2((old - new) * factor)
            accum[h] = accum[h] * rescale + jnp.dot(weights, vals, preferred_element_type=jnp.float32)
            top[h] = jnp.broadcast_to(new, (tok, width))

    pl.when(me + nearest >= first)(add)


def attend(where, queries, starts, arrays, plan, state, finish=False):
    heads, tok, width = queries.shape
    count = len(arrays)
    state_shapes = [
        jax.ShapeDtypeStruct((heads, tok, 2 * width), jnp.float32),
        jax.ShapeDtypeStruct((heads, tok, width), jnp.float32),
    ]
    out_shape = state_shapes
    if finish:
        out_shape = [jax.ShapeDtypeStruct((tok, heads * width), jnp.bfloat16)]
    vmem = pl.BlockSpec(memory_space=pltpu.VMEM)
    given = [] if state is None else list(state)
    keys_seen = 8 * tok

    def kernel(where_ref, q_ref, starts_ref, *refs):
        if finish:
            accum_in, top_in, out_ref, accum, top = refs[count:]
            accum[...] = accum_in[...]
            top[...] = top_in[...]
        else:
            accum, top = refs[-2:]
        if state is None:
            accum[...] = jnp.zeros_like(accum)
            top[...] = jnp.full_like(top, NEG)
        for blocks, nearest, causal in plan(where_ref, refs[:count]):
            visit(where_ref, q_ref, starts_ref, blocks, nearest, accum, top, causal)
        if finish:
            for h in range(heads):
                out_ref[:, h * width : (h + 1) * width] = (
                    accum[h][:, :width] / accum[h][:, width:]
                ).astype(jnp.bfloat16)

    return pl.pallas_call(
        kernel,
        out_shape=out_shape,
        in_specs=[pl.BlockSpec(memory_space=pltpu.SMEM)] + [vmem] * (2 + count + len(given)),
        out_specs=[vmem] * len(out_shape),
        input_output_aliases={} if finish or state is None else {3 + count: 0, 4 + count: 1},
        scratch_shapes=[pltpu.VMEM(shape.shape, jnp.float32) for shape in state_shapes] if finish else [],
        compiler_params=pltpu.CompilerParams(vmem_limit_bytes=16 * 1024 * 1024),
        cost_estimate=pl.CostEstimate(
            flops=4 * heads * tok * keys_seen * width,
            bytes_accessed=4 * keys_seen * width,
            transcendentals=heads * tok * keys_seen,
        ),
        name="attend",
    )(where, queries, starts, *arrays, *given)


def project(where, attended, weights, partial=None):
    tok, _ = attended.shape
    cols = weights[0][0].shape[0]
    given = [] if partial is None else [partial]

    def kernel(where_ref, attended_ref, *refs):
        weight_refs, out_ref = refs[: len(weights)], refs[-1]
        core, plane = where_ref[3], where_ref[0] // 8
        for weight_ref, (_, distance) in zip(weight_refs, weights):
            owner = lax.rem(plane + 8 - distance, 8)
            out_ref[jnp.bitwise_xor(owner & 1, core), owner >> 1] = lax.dot_general(
                attended_ref[...], weight_ref[...], (((1,), (1,)), ((), ())), preferred_element_type=jnp.float32
            ).astype(jnp.bfloat16)

    vmem = pl.BlockSpec(memory_space=pltpu.VMEM)
    return pl.pallas_call(
        kernel,
        out_shape=jax.ShapeDtypeStruct((2, 4, tok, cols), jnp.bfloat16),
        in_specs=[pl.BlockSpec(memory_space=pltpu.SMEM)] + [vmem] * (1 + len(weights) + len(given)),
        out_specs=vmem,
        input_output_aliases={2 + len(weights): 0} if given else {},
        compiler_params=pltpu.CompilerParams(vmem_limit_bytes=16 * 1024 * 1024),
        name="project",
    )(where, attended, *[weight for weight, _ in weights], *given)


def down_column(array, steps):
    return lax.ppermute(
        array, "seq", [(8 * z + y, 8 * ((z + steps) % 8) + y) for z in range(8) for y in range(8)]
    )


def along_row(array, steps):
    return lax.ppermute(
        array, "seq", [(8 * z + y, 8 * z + (y + steps) % 8) for z in range(8) for y in range(8)]
    )


def layer(queries, keys, values, out_weight, doc_lengths):
    tok, _, width = queries.shape
    me = lax.axis_index("seq")
    core = lax.axis_index("head") % 2

    own = jnp.concatenate([keys.reshape(1, tok, width), values.reshape(1, tok, width)], axis=1)
    near = down_column(own, 1)
    far = down_column(own, 4)
    two = jnp.concatenate([own, near], axis=0)
    double = down_column(two, 2)
    column = jnp.concatenate([two, double, far], axis=0)
    turned = out_weight.T
    weight = lax.all_to_all(
        jnp.broadcast_to(turned[None], (8,) + turned.shape),
        "seq",
        0,
        0,
        axis_index_groups=[[8 * z + y for y in range(8)] for z in range(8)],
        tiled=True,
    ).reshape(8 * turned.shape[0], turned.shape[1])
    ends = jnp.cumsum(doc_lengths)
    position = me * tok + jnp.arange(tok, dtype=jnp.int32)
    starts = jnp.max(jnp.where(ends[None, :] <= position[:, None], ends[None, :], 0), axis=1)
    where = jnp.stack([me, starts[0] // tok, starts[-1], core]).astype(jnp.int32)
    starts = jnp.broadcast_to(starts[:, None], (tok, 128))
    queries = jnp.transpose(queries, (1, 0, 2))


    def own_plan(where_ref, refs):
        me = where_ref[0]
        yield [(refs[0], a, me - 8 * a) for a in range(4)], 0, True

    def turn_plan(turn):
        def plan(where_ref, refs):
            me = where_ref[0]
            place = lax.rem(me, 8)
            skip = jnp.where(place >= turn, 0, 1)
            yield [(refs[0], skip + a, me - turn - 8 * a) for a in range(4)], -turn, False
            skip = jnp.where(place + turn < 8, 1, 0)
            yield [(refs[1], skip + a, me + turn - 8 - 8 * a) for a in range(4)], turn - 8, False

        return plan

    def last_plan(where_ref, refs):
        me = where_ref[0]
        place = lax.rem(me, 8)
        up, down, column, first_up, edge = refs
        shift = jnp.where(place >= 4, -4, 4)
        numbers = [me + shift - 8 * a for a in range(5)]
        numbers = [jnp.where(number > me, -1, number) for number in numbers]
        blocks = [(up, a, numbers[a]) for a in range(3)] + [(down, a, numbers[3 + a]) for a in range(2)]
        yield blocks, -4, False
        beyond = jnp.where(place > 0, me - 33, -1)
        blocks = [(column, 4, me - 32), (first_up, 4, beyond), (edge, 0, jnp.where(place > 0, -1, me - 33))]
        yield blocks, -32, False

    state, arrays, plan = None, [column], own_plan
    up = down = column
    ahead = behind = weight
    weights = [(weight, 0)]
    for turn in range(1, 5):
        up = along_row(up if turn < 4 else up[:3], 1)
        down = along_row(down if turn < 4 else down[3:], -1)
        if turn == 1:
            first_up = up
        state = attend(where, queries, starts, arrays, plan, state)
        behind = down_column(behind, -1)
        weights.append((behind, 8 - turn))
        if turn < 4:
            ahead = down_column(ahead, 1)
            weights.append((ahead, turn))
        arrays, plan = [up, down], turn_plan(turn)
    edge = lax.ppermute(column[:1], "seq", [(8 * z + 7, 8 * ((z + 5) % 8)) for z in range(8)])
    arrays = [up, down, column, first_up, edge]
    (attended,) = attend(where, queries, starts, arrays, last_plan, state, True)
    partial = project(where, attended, weights[:6])
    partial = project(where, attended, weights[6:], partial)

    other = lax.ppermute(partial[1], "head", [(h, h ^ 1) for h in range(8)])
    both = (partial[0].astype(jnp.float32) + other.astype(jnp.float32)).astype(jnp.bfloat16)
    parts = lax.all_to_all(
        both, "head", 0, 0, axis_index_groups=[[0, 2, 4, 6], [1, 3, 5, 7]], tiled=True
    )
    return jnp.sum(parts.astype(jnp.float32), axis=0).astype(jnp.bfloat16)


def solution(mesh):
    placed = (
        P("seq", "head", None),
        P("seq", "head", None),
        P("seq", "head", None),
        P("head", "seq"),
        P(),
    )
    return jax.shard_map(layer, mesh=mesh, in_specs=placed, out_specs=P("seq", "head"), check_vma=False)
```
